512 devices in a mesh: seq: 32 (over z, y_lo), tp: 16 (over x, y_hi, core).
Axes of the slice: x: 4, y: 4 (y_hi: 2, y_lo: 2; y = y_hi * 2 + y_lo), z: 16, core: 2. Of those that a mesh axis runs over, the one named last changes fastest.
Arguments:
- inputs: bfloat16 [2, 128, 8192], P(None, 'seq', 'tp'), may hold values from -6 to 6
- out_grad: bfloat16 [2, 128, 8192], P(None, 'seq', 'tp'), may hold values from -6 to 6
- gate_weight: bfloat16 [8192, 14848], P('tp', 'seq'), may hold values from -0.0625 to 0.0625
- up_weight: bfloat16 [8192, 14848], P('tp', 'seq'), may hold values from -0.0625 to 0.0625
- down_weight: bfloat16 [14848, 8192], P('seq', 'tp'), may hold values from -0.0625 to 0.0625
Outputs:
- input_grad: bfloat16 [2, 128, 8192], P(None, 'seq', 'tp')
- gate_grad: float32 [8192, 14848], P('tp', 'seq')
- up_grad: float32 [8192, 14848], P('tp', 'seq')
- down_grad: float32 [14848, 8192], P('seq', 'tp')
The draws below stay inside these ranges and needn't reach their ends.
All inputs are finite; a program needn't handle non-finite values.
Results may differ from the reference program's by a relative error of at most 0.0049.
Values may be sent and summed in bfloat16 or wider, within the bound.
A program may use at most 64 MiB of HBM per device.

```python
import jax
import jax.numpy as jnp

D = 8192
FFW = 14848
GROUPS = 2
TC = 128


def steps_of(rng, shape, pieces, least, high):
    factor_of = 1.0
    for axis_at, shards_of in pieces:
        draws = jax.random.uniform(jax.random.fold_in(jax.random.fold_in(rng, 6), axis_at), (shards_of,), jnp.float32, least / len(pieces), high / len(pieces))
        factor_of = factor_of * jnp.repeat(jnp.exp(draws), shape[axis_at] // shards_of).reshape((-1,) + (1,) * (len(shape) - 1 - axis_at))
    return factor_of


def normal_values(own_key, dims, scale, bound, shards=(), kind=jnp.bfloat16):
    array = jax.random.normal(own_key, dims, jnp.float32) * scale
    if len(shards) > 0:
        array = steps_of(own_key, dims, shards, -0.22, 0.18) * array
    return jnp.clip(array, min=-bound, max=bound).astype(kind)


def setup_inputs(seed: int = 0) -> dict:
    key_of = jax.random.split(jax.random.key(seed), 6)
    return {
        "inputs": normal_values(key_of[0], (GROUPS, TC, D), 1.0, 6.0, ((1, 32), (2, 16))),
        "out_grad": normal_values(key_of[1], (GROUPS, TC, D), 1.0, 6.0, ((1, 32), (2, 16))),
        "gate_weight": normal_values(key_of[2], (D, FFW), D ** -0.5, 0.0625, ((0, 16), (1, 32))),
        "up_weight": normal_values(key_of[3], (D, FFW), D ** -0.5, 0.0625, ((0, 16), (1, 32))),
        "down_weight": normal_values(key_of[4], (FFW, D), D ** -0.5, 0.0625, ((0, 32), (1, 16))),
    }


def reference(inputs, out_grad, gate_weight, up_weight, down_weight):
    gate_total = jnp.zeros((D, FFW), jnp.float32)
    up_total = jnp.zeros((D, FFW), jnp.float32)
    down_total = jnp.zeros((FFW, D), jnp.float32)
    results = []
    for index in range(GROUPS):
        block_in = inputs[index]
        block_grad = out_grad[index]
        gate = jnp.dot(block_in, gate_weight, preferred_element_type=jnp.float32)
        up_proj = jnp.dot(block_in, up_weight, preferred_element_type=jnp.float32)
        hidden = (jax.nn.silu(gate) * up_proj).astype(jnp.bfloat16)
        hidden_grad = jnp.dot(block_grad, down_weight.T, preferred_element_type=jnp.float32)
        sig = jax.nn.sigmoid(gate)
        up_unit = (hidden_grad * gate * sig).astype(jnp.bfloat16)
        gate_unit = (hidden_grad * up_proj * sig * (1.0 + gate * (1.0 - sig))).astype(jnp.bfloat16)
        grad_in = jnp.dot(gate_unit, gate_weight.T, preferred_element_type=jnp.float32)
        grad_in = grad_in + jnp.dot(up_unit, up_weight.T, preferred_element_type=jnp.float32)
        results.append(grad_in.astype(jnp.bfloat16))
        gate_total = gate_total + jnp.dot(block_in.T, gate_unit, preferred_element_type=jnp.float32)
        up_total = up_total + jnp.dot(block_in.T, up_unit, preferred_element_type=jnp.float32)
        down_total = down_total + jnp.dot(hidden.T, block_grad, preferred_element_type=jnp.float32)
    return jnp.stack(results), gate_total, up_total, down_total
```

```python
import jax
import jax.numpy as jnp
from jax import lax
from jax.experimental import pallas as pl
from jax.experimental.pallas import tpu as pltpu
from jax.sharding import PartitionSpec as P

MESH = pl.DeviceIdType.MESH
F32, BF16 = jnp.float32, jnp.bfloat16

SPREAD = {0: (3, -3, 1, -1), -3: (3, 1, -1), 3: (-3, -1, 1), -6: (2, 1, -1), 6: (-2, -1, 1)}
LABELS = (-1, 1, -3, 3, -4, -2, 2, 4, -6, 6, -7, -5, 5, 7, -8, 8)
PARENT = {1: 0, -1: 0, 2: 3, 4: 3, -2: -3, -4: -3, 5: 6, 7: 6, -5: -6, -7: -6, 8: 6, -8: -6,
          6: 3, -6: -3, 3: 0, -3: 0}
LEAVES = (8, -8, 7, -7, 5, -5, 4, -4, 2, -2, 1, -1)
CHILDREN = {6: (5, 7, 8), -6: (-5, -7, -8), 3: (2, 4, 6), -3: (-2, -4, -6), 0: (1, -1, 3, -3)}
Y_ORDER = (8, 7, -7, 5, -5, 6, -6, 4, -4, 2, -2, 3, -3, 1, -1, 0)


def kernel(nz, nx, x_ref, dy_ref, wg_any, wu_any, wd_any, dx_ref, gg_any, ug_any, dg_any,
           buf, wg, wu, wd, xs, ys, own, far, got, slabs, landed, act,
           dxp, ysend, yrecv, zsend, zrecv, gg, ug, dg,
           load_sem, store_sem, zs_sem, zr_sem, ys_sem, yr_sem, cs_sem, cr_sem,
           ts_sem, tr_sem, as_sem, ar_sem, bs_sem, br_sem, fys_sem, fyr_sem, fzs_sem, fzr_sem):
    s = lax.axis_index("seq")
    t = lax.axis_index("tp")
    z, yl = s // 2, s % 2
    core, yh, x = t % 2, (t // 2) % 2, t // 4

    def seq_at(dz, flip=0):
        return lax.rem(z + dz + nz, nz) * 2 + (yl if flip == 0 else 1 - yl)

    def chip_at(dx, dyh):
        return lax.rem(x + dx + nx, nx) * 2 + lax.rem(yh + dyh, 2)

    others = [(2, 1), (1, 1), (3, 1), (2, 0), (0, 1), (1, 0), (3, 0)]

    def copy_to(src, dst, send, recv, device):
        return pltpu.make_async_remote_copy(
            src_ref=src, dst_ref=dst, send_sem=send, recv_sem=recv, device_id=device,
            device_id_type=MESH)

    mate = (s, t + 1 - 2 * core)
    across = (seq_at(0, 1), t)
    barrier = pltpu.get_barrier_semaphore()
    partners = [(seq_at(d), t) for d in (3, -3, 2, -2, 1, -1)] + [across, mate]
    partners += [(s, chip_at(*k) * 2 + core) for k in others]
    for device in partners:
        pl.semaphore_signal(barrier, inc=1, device_id=device, device_id_type=MESH)
    loads = [pltpu.make_async_copy(a, b, load_sem.at[i])
             for i, (a, b) in enumerate(((wg_any, wg), (wu_any, wu), (wd_any, wd)))]
    for c in loads:
        c.start()
    rows, depth = buf.shape[2], buf.shape[3]
    buf[s, 0] = x_ref[...].reshape(rows, depth)
    buf[s, 1] = dy_ref[...].reshape(rows, depth)
    pl.semaphore_wait(barrier, len(partners))

    sent = []

    def send(*a):
        c = copy_to(*a)
        c.start()
        sent.append(c)

    def part(o, label):
        ref = buf.at[seq_at(o)]
        if label == -8:
            return ref.at[0]
        if label == 8:
            return ref.at[1]
        return ref

    count = [0]

    def pass_on(o):
        for d in SPREAD.get(o, ()):
            label = o - d
            send(part(o, label), part(o, label), zs_sem.at[count[0]], zr_sem.at[label + 8],
                 (seq_at(d), t))
            count[0] += 1
        if abs(o) == 8:
            piece = part(8, o)
            send(piece, piece, ys_sem.at[o + 8], yr_sem.at[o + 8], across)
        else:
            send(buf.at[seq_at(o)], buf.at[seq_at(o)], ys_sem.at[o + 8], yr_sem.at[o + 8], across)

    pass_on(0)
    for label in LABELS:
        piece = part(label, label)
        copy_to(piece, piece, zs_sem.at[0], zr_sem.at[label + 8], across).wait_recv()
        pass_on(label)
    for label in (0,) + LABELS:
        ref = buf.at[seq_at(label, 1)]
        piece = ref.at[0] if label == -8 else ref.at[1] if label == 8 else ref
        copy_to(piece, piece, ys_sem.at[0], yr_sem.at[label + 8], across).wait_recv()
    xs[...] = buf[:, 0].astype(F32).reshape(xs.shape).astype(BF16)
    ys[...] = buf[:, 1].astype(F32).reshape(ys.shape).astype(BF16)
    for c in loads:
        c.wait()

    half = xs.shape[0] // 2
    mine = pl.ds(pl.multiple_of(core * half, half), half)
    theirs = pl.ds(pl.multiple_of((1 - core) * half, half), half)
    last = (((1,), (1,)), ((), ()))

    def product(k, at):
        rows_of, weight = ((xs, wg), (xs, wu), (ys, wd))[k]
        return lax.dot_general(rows_of[at, :], weight[...], last, preferred_element_type=F32)

    for k in range(3):
        far[k] = product(k, theirs)
        send(far.at[k], got.at[k], cs_sem.at[k], cr_sem.at[k], mate)
    for k in range(3):
        own[k] = product(k, mine)
    chips = slabs.shape[0]
    share = half // chips
    for k in range(3):
        copy_to(far.at[k], got.at[k], cs_sem.at[k], cr_sem.at[k], mate).wait_recv()
        total = own[k] + got[k]
        own[k] = total
        slabs[:, k] = total.reshape(chips, share, -1).astype(BF16)
    for i, k in enumerate(others):
        chip = chip_at(*k)
        send(slabs.at[chip], landed.at[i], ts_sem.at[i], tr_sem.at[i], (s, chip * 2 + core))
    me = chip_at(0, 0)
    sums = [own[k, pl.ds(pl.multiple_of(me * share, share), share), :] for k in range(3)]
    for i in range(len(others)):
        copy_to(slabs.at[0], landed.at[i], ts_sem.at[i], tr_sem.at[i], mate).wait_recv()
        for k in range(3):
            sums[k] = sums[k] + landed[i, k].astype(F32)
    gate, up, grad = sums
    sig = jax.nn.sigmoid(gate)
    silu = gate * sig
    at = core * chips + me
    act[at, 0] = (silu * up).astype(BF16)
    act[at, 1] = (grad * gate * sig).astype(BF16)
    act[at, 2] = (grad * up * sig * (1.0 + gate * (1.0 - sig))).astype(BF16)

    for i, k in enumerate(others):
        send(act.at[at], act.at[at], as_sem.at[i], ar_sem.at[i], (s, chip_at(*k) * 2 + core))
    send(act.at[at], act.at[at], bs_sem.at[7], br_sem.at[7], mate)
    for i, (a, b) in enumerate(others):
        from_chip = core * chips + chip_at(-a, b)
        ref = act.at[from_chip]
        copy_to(ref, ref, as_sem.at[i], ar_sem.at[i], mate).wait_recv()
        send(ref, ref, bs_sem.at[i], br_sem.at[i], mate)
    for i, (a, b) in list(enumerate(others)) + [(7, (0, 0))]:
        ref = act.at[(1 - core) * chips + chip_at(-a, b)]
        copy_to(ref, ref, bs_sem.at[i], br_sem.at[i], mate).wait_recv()

    tokens, units = xs.shape[0], wg.shape[0]
    gate_unit = act[:, 2].reshape(tokens, units)
    up_unit = act[:, 1].reshape(tokens, units)
    term = jnp.dot(gate_unit, wg[...], preferred_element_type=F32)
    term = term + jnp.dot(up_unit, wu[...], preferred_element_type=F32)
    dxp[...] = term.reshape(dxp.shape)

    for i, o in enumerate(Y_ORDER):
        ysend[i] = dxp[seq_at(-o, 1)].astype(BF16)
        send(ysend.at[i], yrecv.at[i], fys_sem.at[i], fyr_sem.at[i], across)

    first = (((0,), (0,)), ((), ()))
    gg[...] = lax.dot_general(gate_unit, xs[...], first, preferred_element_type=F32)
    ug[...] = lax.dot_general(up_unit, xs[...], first, preferred_element_type=F32)
    stores = [pltpu.make_async_copy(gg, gg_any, store_sem.at[0]),
              pltpu.make_async_copy(ug, ug_any, store_sem.at[1])]
    for c in stores:
        c.start()

    def column_term(o):
        i = Y_ORDER.index(8 if o == -8 else o)
        return dxp[seq_at(-o)] + yrecv[i].astype(F32)

    waited = set()

    def wait_y(o):
        i = Y_ORDER.index(8 if o == -8 else o)
        if i not in waited:
            waited.add(i)
            copy_to(ysend.at[i], yrecv.at[i], fys_sem.at[i], fyr_sem.at[i], across).wait_recv()

    wide = depth // 2

    def piece_of(ref, o):
        if o == 8:
            return ref.at[16, :, pl.ds(0, wide)]
        if o == -8:
            return ref.at[17, :, pl.ds(0, wide)]
        return ref.at[o + 8]

    def give(o, value):
        if o == 8:
            zsend[16, :, :wide] = value[:, :wide]
        elif o == -8:
            zsend[17, :, :wide] = value[:, wide:]
        else:
            zsend[o + 8] = value
        send(piece_of(zsend, o), piece_of(zrecv, o), fzs_sem.at[o + 8], fzr_sem.at[o + 8],
             (seq_at(PARENT[o] - o), t))

    def collected(o):
        wait_y(o)
        value = column_term(o)
        for c in CHILDREN[o]:
            ref = piece_of(zrecv, c)
            copy_to(ref, ref, fzs_sem.at[0], fzr_sem.at[c + 8], across).wait_recv()
        for c in CHILDREN[o]:
            if c == 8:
                value = value + jnp.concatenate(
                    [zrecv[16, :, :wide], jnp.zeros((rows, wide), F32)], axis=1)
            elif c == -8:
                value = value + jnp.concatenate(
                    [jnp.zeros((rows, wide), F32), zrecv[17, :, :wide]], axis=1)
            else:
                value = value + zrecv[c + 8]
        return value

    for o in LEAVES:
        wait_y(o)
        give(o, column_term(o))
    dg[...] = lax.dot_general(act[:, 0].reshape(tokens, units), ys[...], first,
                              preferred_element_type=F32)
    c = pltpu.make_async_copy(dg, dg_any, store_sem.at[2])
    c.start()
    stores.append(c)
    for o in (6, -6, 3, -3):
        give(o, collected(o))
    dx_ref[...] = collected(0).astype(BF16)

    for c in sent:
        c.wait_send()
    for c in stores:
        c.wait()


def solution(mesh):
    nz = mesh.shape["seq"] // 2
    nx = mesh.shape["tp"] // 4
    chips = mesh.shape["tp"] // 2

    def per_device(inputs, out_grad, gate_weight, up_weight, down_weight):
        groups, local, depth = inputs.shape
        rows = groups * local
        units = gate_weight.shape[1]
        tokens = rows * mesh.shape["seq"]
        half, share = tokens // 2, tokens // (2 * chips)
        whole = pl.BlockSpec(memory_space=pltpu.VMEM)
        anywhere = pl.BlockSpec(memory_space=pl.ANY)
        dma = pltpu.SemaphoreType.DMA
        vmem = pltpu.VMEM
        out = pl.pallas_call(
            lambda *refs: kernel(nz, nx, *refs),
            out_shape=(
                jax.ShapeDtypeStruct((rows, depth), BF16),
                jax.ShapeDtypeStruct((units, depth), F32),
                jax.ShapeDtypeStruct((units, depth), F32),
                jax.ShapeDtypeStruct((units, depth), F32),
            ),
            in_specs=[whole, whole, anywhere, anywhere, anywhere],
            out_specs=(whole, anywhere, anywhere, anywhere),
            scratch_shapes=[
                vmem((2 * nz, 2, rows, depth), BF16),
                vmem((units, depth), BF16), vmem((units, depth), BF16), vmem((units, depth), BF16),
                vmem((tokens, depth), BF16), vmem((tokens, depth), BF16),
                vmem((3, half, units), F32), vmem((3, half, units), F32),
                vmem((3, half, units), F32),
                vmem((chips, 3, share, units), BF16),
                vmem((chips - 1, 3, share, units), BF16),
                vmem((2 * chips, 3, share, units), BF16),
                vmem((2 * nz, rows, depth), F32),
                vmem((nz, rows, depth), BF16), vmem((nz, rows, depth), BF16),
                vmem((18, rows, depth), F32), vmem((18, rows, depth), F32),
                vmem((units, depth), F32), vmem((units, depth), F32), vmem((units, depth), F32),
                dma((3,)), dma((3,)),
                dma((16,)), dma((17,)), dma((17,)), dma((17,)),
                dma((3,)), dma((3,)),
                dma((7,)), dma((7,)), dma((7,)), dma((7,)), dma((8,)), dma((8,)),
                dma((16,)), dma((16,)), dma((17,)), dma((17,)),
            ],
            compiler_params=pltpu.CompilerParams(
                collective_id=0, has_side_effects=True, vmem_limit_bytes=48 * 2**20),
        )(inputs, out_grad, gate_weight.T, up_weight.T, down_weight)
        return out[0].reshape(groups, local, depth), out[1].T, out[2].T, out[3]

    return jax.shard_map(
        per_device, mesh=mesh,
        in_specs=(P(None, "seq", "tp"), P(None, "seq", "tp"), P("tp", "seq"), P("tp", "seq"),
                  P("seq", "tp")),
        out_specs=(P(None, "seq", "tp"), P("tp", "seq"), P("tp", "seq"), P("seq", "tp")),
        check_vma=False)
```

```python
import functools

import jax
import jax.numpy as jnp
from jax import lax
from jax.experimental import pallas as pl
from jax.experimental.pallas import tpu as pltpu
from jax.sharding import PartitionSpec as P

MESH = pl.DeviceIdType.MESH
F32, BF16 = jnp.float32, jnp.bfloat16

FAR_Y = (0, 1, "M")


def onward(core, oz):
    far = "M" if core else "R"
    here = () if core else ((0, 0, "M"),)
    sign = 1 if oz > 0 else -1
    near = ((1, 0, "M"), (-1, 0, "M"))
    if oz == 0:
        return ((3, 0, far), (-3, 0, far)) + near + (FAR_Y,)
    if abs(oz) == 3:
        return ((3 * sign, 0, far),) + near + here + (FAR_Y,)
    if abs(oz) == 6:
        return ((2 * sign, 1, "M"), (2 * sign, 0, "M"), (1, 1, "M"), (-1, 1, "M")) + near + here + (FAR_Y,)
    return (FAR_Y,) if abs(oz) in (1, 2, 4) else ()


def carrier(core, oz):
    return 1 if core or abs(oz) in (3, 6) else 0


INNER = (0, 1, -1, 3, -3, 2, -2, 4, -4, 6, -6)
EDGES = [(core, oz, dz, dy, kind) for core in (1, 0) for oz in INNER for dz, dy, kind in onward(core, oz)]
UP = {(core, oz + dz, dy, kind): (oz, dz, dy) for core, oz, dz, dy, kind in EDGES}


def is_inner(core, oz, dy, kind):
    return dy == 0 and oz in INNER and (kind == "R" or carrier(core, oz) == core)


LEAF_KEYS = [k for k in UP if not is_inner(*k)]
INNER_KEYS = [k for k in UP if is_inner(*k)]
HELD = [k for k in dict.fromkeys((oz + dz, dy) for _, oz, dz, dy, kind in EDGES if kind == "M")]
RELAYED = [3, -3, 6, -6]


def kernel(nz, nx, x_any, dy_any, wg_any, wu_any, wd_any, dx_ref, gg, ug, dg,
           xin, dyin, buf, relay, wg, wu, wd, xs, ys, own, far, got, slabs, landed, act,
           dxp, leaves, lrecv, zsend, zrecv,
           load_sem, zs_sem, zr_sem, rr_sem, cs_sem, cr_sem,
           ts_sem, tr_sem, as_sem, ar_sem, bs_sem, br_sem, fys_sem, fyr_sem, fzs_sem, fzr_sem):
    s = lax.axis_index("seq")
    t = lax.axis_index("tp")
    z, yl = s // 2, s % 2
    core, yh, x = t % 2, (t // 2) % 2, t // 4

    along = {(d, f): lax.rem(z + d + nz, nz) * 2 + (1 - yl if f else yl) for d in range(-8, 9) for f in (0, 1)}
    def seq_at(dz, flip=0):
        return along[dz, flip]

    def chip_at(dx, dyh):
        return lax.rem(x + dx + nx, nx) * 2 + lax.rem(yh + dyh, 2)

    others = [(2, 1), (1, 1), (3, 1), (2, 0), (0, 1), (1, 0), (3, 0)]

    def copy_to(src, dst, send, recv, device):
        return pltpu.make_async_remote_copy(
            src_ref=src, dst_ref=dst, send_sem=send, recv_sem=recv, device_id=device,
            device_id_type=MESH)

    mate = (s, t + 1 - 2 * core)
    across = (seq_at(0, 1), t)
    barrier = pltpu.get_barrier_semaphore()
    on_core = (t - core, t - core + 1)

    def met_by(c):
        met = {(0, 0, 1 - c)}
        for owner, oz, dz, dy, kind in EDGES:
            a, b = carrier(owner, oz), 1 if kind == "R" else owner
            met |= {(dz, dy, b)} if a == c else set()
            met |= {(-dz, dy, a)} if b == c else set()
        return sorted(met - {(0, 0, c)}, key=lambda m: (-abs(m[0]), m))

    def greet(c):
        partners = [(along[d, f], on_core[k]) for d, f, k in met_by(c)]
        partners += [(s, chip * 2 + core) for chip in chips_at]
        for device in partners:
            pl.semaphore_signal(barrier, inc=1, device_id=device, device_id_type=MESH)

    def greeted(c):
        pl.semaphore_wait(barrier, len(met_by(c)) + len(others))

    def on_cores(body):
        for c in (1, 0):
            pl.when(core == c)(functools.partial(body, c))

    chips_at = [chip_at(*k) for k in others]
    loads = [pltpu.make_async_copy(a, b, load_sem.at[i])
             for i, (a, b) in enumerate(((x_any, xin), (dy_any, dyin), (wg_any, wg), (wu_any, wu), (wd_any, wd)))]
    for c in loads[:2]:
        c.start()
    on_cores(greet)
    rows, depth = buf.shape[2], buf.shape[3]
    for c in loads[:2]:
        c.wait()
    buf[s, 0] = xin[...].reshape(rows, depth)
    buf[s, 1] = dyin[...].reshape(rows, depth)
    for c in loads[2:]:
        c.start()
    on_cores(greeted)

    sent = []

    def done():
        for c in sent:
            c.wait_send()
        for k in (0, 1):
            @pl.when(core == k)
            def _(k=k):
                for make in later[k]:
                    make().wait_send()

    def send(*a):
        c = copy_to(*a)
        c.start()
        sent.append(c)

    later = {0: [], 1: []}

    def tp_of(c):
        return on_core[c]

    def issue(c, make):
        make().start()
        later[c].append(make)

    def half_of(ref, oz):
        return ref.at[0] if oz == 8 else ref.at[1] if oz == -8 else ref

    def held(oz, dy):
        return half_of(buf.at[seq_at(-oz, dy)], oz)

    def pass_on(c, oz, kind, by):
        for dz, dy, to in onward(c, oz):
            n = EDGES.index((c, oz, dz, dy, to))
            far = oz + dz

            def make(dz=dz, dy=dy, to=to, n=n, far=far):
                src = relay.at[RELAYED.index(oz)] if kind == "R" else buf.at[seq_at(-oz)]
                dst = relay.at[RELAYED.index(far)] if to == "R" else buf.at[seq_at(-oz)]
                sem = rr_sem.at[RELAYED.index(far)] if to == "R" else zr_sem.at[HELD.index((far, dy))]
                return copy_to(half_of(src, far), half_of(dst, far), zs_sem.at[n], sem,
                               (seq_at(dz, dy), tp_of(1 if to == "R" else c)))
            issue(by, make)

    def arrived(oz, dy):
        ref = held(oz, dy)
        copy_to(ref, ref, zs_sem.at[0], zr_sem.at[HELD.index((oz, dy))], across).wait_recv()

    def relay_arrived(oz):
        i = RELAYED.index(oz)
        copy_to(relay.at[i], relay.at[i], zs_sem.at[0], rr_sem.at[i], across).wait_recv()

    @pl.when(core == 1)
    def _():
        pass_on(1, 0, "M", 1)
        for oz in (1, -1):
            arrived(oz, 0)
            pass_on(1, oz, "M", 1)
        for oz in (3, -3):
            arrived(oz, 0)
            pass_on(1, oz, "M", 1)
        for oz in (3, -3):
            relay_arrived(oz)
            pass_on(0, oz, "R", 1)
        for oz in (2, -2, 4, -4):
            arrived(oz, 0)
            pass_on(1, oz, "M", 1)
        for oz in (6, -6):
            arrived(oz, 0)
            pass_on(1, oz, "M", 1)
        for oz in (6, -6):
            relay_arrived(oz)
            pass_on(0, oz, "R", 1)
        for oz, dy in HELD:
            if dy or oz not in INNER:
                arrived(oz, dy)

    @pl.when(core == 0)
    def _():
        pass_on(0, 0, "M", 0)
        for oz in (1, -1, 2, -2, 4, -4):
            arrived(oz, 0)
            pass_on(0, oz, "M", 0)
        for oz, dy in HELD:
            if dy or oz not in (0, 1, -1, 2, -2, 4, -4):
                arrived(oz, dy)

    xs[...] = buf[:, 0].astype(F32).reshape(xs.shape).astype(BF16)
    ys[...] = buf[:, 1].astype(F32).reshape(ys.shape).astype(BF16)
    for c in loads[2:]:
        c.wait()

    half = xs.shape[0] // 2
    mine = pl.ds(pl.multiple_of(core * half, half), half)
    theirs = pl.ds(pl.multiple_of((1 - core) * half, half), half)
    last = (((1,), (1,)), ((), ()))

    def product(k, at):
        rows_of, weight = ((xs, wg), (xs, wu), (ys, wd))[k]
        return lax.dot_general(rows_of[at, :], weight[...], last, preferred_element_type=F32)

    chips = slabs.shape[1]
    share = half // chips
    for k in range(3):
        far[k] = product(k, theirs)
        send(far.at[k], got.at[k], cs_sem.at[k], cr_sem.at[k], mate)
    own[0] = product(0, mine)
    for k in range(3):
        copy_to(far.at[k], got.at[k], cs_sem.at[k], cr_sem.at[k], mate).wait_recv()
        total = own[k] + got[k]
        own[k] = total
        slabs[k] = total.reshape(chips, share, -1).astype(BF16)
        for i, (a, b) in enumerate(others):
            chip = chip_at(a, b)
            send(slabs.at[k, chip], landed.at[i, k], ts_sem.at[i, k], tr_sem.at[i, k],
                 (s, chip * 2 + core))
        if k < 2:
            own[k + 1] = product(k + 1, mine)
    me = chip_at(0, 0)
    sums = [own[k, pl.ds(pl.multiple_of(me * share, share), share), :] for k in range(3)]
    for k in range(3):
        for i in range(len(others)):
            copy_to(slabs.at[k, 0], landed.at[i, k], ts_sem.at[i, k], tr_sem.at[i, k], mate).wait_recv()
            sums[k] = sums[k] + landed[i, k].astype(F32)
    gate, up, grad = sums
    sig = jax.nn.sigmoid(gate)
    silu = gate * sig
    at = core * chips + me
    act[at, 0] = (silu * up).astype(BF16)
    act[at, 1] = (grad * gate * sig).astype(BF16)
    act[at, 2] = (grad * up * sig * (1.0 + gate * (1.0 - sig))).astype(BF16)

    for i, k in enumerate(others):
        send(act.at[at], act.at[at], as_sem.at[i], ar_sem.at[i], (s, chip_at(*k) * 2 + core))
    send(act.at[at], act.at[at], bs_sem.at[7], br_sem.at[7], mate)
    for i, (a, b) in enumerate(others):
        from_chip = core * chips + chip_at(-a, b)
        ref = act.at[from_chip]
        copy_to(ref, ref, as_sem.at[i], ar_sem.at[i], mate).wait_recv()
        send(ref, ref, bs_sem.at[i], br_sem.at[i], mate)
    for i, (a, b) in list(enumerate(others)) + [(7, (0, 0))]:
        ref = act.at[(1 - core) * chips + chip_at(-a, b)]
        copy_to(ref, ref, bs_sem.at[i], br_sem.at[i], mate).wait_recv()

    tokens, units = xs.shape[0], wg.shape[0]
    gate_unit = act[:, 2].reshape(tokens, units)
    up_unit = act[:, 1].reshape(tokens, units)
    term = jnp.dot(gate_unit, wg[...], preferred_element_type=F32)
    term = term + jnp.dot(up_unit, wu[...], preferred_element_type=F32)
    dxp[...] = term.reshape(dxp.shape)

    leaves[...] = term.reshape(dxp.shape).astype(BF16)
    first = (((0,), (0,)), ((), ()))
    wide = depth // 2

    def side(ref, oz):
        return ref.at[:, pl.ds(0, wide)] if oz == 8 else ref.at[:, pl.ds(wide, wide)] if oz == -8 else ref

    def send_up(key, by):
        c, oz, dy, kind = key
        up, dz, _ = UP[key]
        target = (seq_at(-dz, dy), tp_of(carrier(c, up)))
        if key in INNER_KEYS:
            n = INNER_KEYS.index(key)
            issue(by, lambda: copy_to(zsend.at[n], zrecv.at[n], fzs_sem.at[n], fzr_sem.at[n], target))
        else:
            n = LEAF_KEYS.index(key)
            issue(by, lambda: copy_to(side(leaves.at[seq_at(-oz, dy)], oz), side(lrecv.at[n], oz),
                                      fys_sem.at[n], fyr_sem.at[n], target))

    def collected(c, oz):
        kind = "R" if carrier(c, oz) != c else "M"
        value = jnp.zeros((rows, depth), F32) if kind == "R" else dxp[seq_at(-oz)]
        for dz, dy, to in onward(c, oz):
            key = (c, oz + dz, dy, to)
            if key in INNER_KEYS:
                n = INNER_KEYS.index(key)
                copy_to(zsend.at[n], zrecv.at[n], fzs_sem.at[n], fzr_sem.at[n], across).wait_recv()
                value = value + zrecv[n]
            else:
                n = LEAF_KEYS.index(key)
                ref = side(lrecv.at[n], key[1])
                copy_to(ref, ref, fys_sem.at[n], fyr_sem.at[n], across).wait_recv()
                nothing = jnp.zeros((rows, wide), F32)
                if key[1] == 8:
                    value = value + jnp.concatenate([lrecv[n, :, :wide].astype(F32), nothing], axis=1)
                elif key[1] == -8:
                    value = value + jnp.concatenate([nothing, lrecv[n, :, wide:].astype(F32)], axis=1)
                else:
                    value = value + lrecv[n].astype(F32)
        return value

    def forward(c, oz, by):
        key = (c, oz, 0, "R" if carrier(c, oz) != c else "M")
        zsend[INNER_KEYS.index(key)] = collected(c, oz)
        send_up(key, by)

    urgent = (8, 7, 5, 6, 4, 2, 3, 1, 0)

    def start_leaves(c):
        mine = [k for k in LEAF_KEYS if k[0] == c]
        for key in sorted(mine, key=lambda k: (urgent.index(abs(k[1])), -k[2])):
            send_up(key, c)

    def middle(c):
        for oz in (4, -4, 2, -2, 1, -1):
            forward(c, oz, c)

    def outer(c):
        for oz in (6, -6):
            for b in ((1, 0) if c else ()):
                forward(b, oz, c)

    def finish(c):
        for oz in (3, -3):
            for b in ((1, 0) if c else ()):
                forward(b, oz, c)
        dx_ref[...] = collected(c, 0).astype(BF16)

    on_cores(start_leaves)
    gg[...] = lax.dot_general(gate_unit, xs[...], first, preferred_element_type=F32)
    on_cores(middle)
    on_cores(outer)
    ug[...] = lax.dot_general(up_unit, xs[...], first, preferred_element_type=F32)
    dg[...] = lax.dot_general(act[:, 0].reshape(tokens, units), ys[...], first,
                              preferred_element_type=F32)
    on_cores(finish)

    done()


def write_out(dx, gg, ug, dg, dx_out, gg_out, ug_out, dg_out, staged, sem):
    copies = [pltpu.make_async_copy(a, b, sem.at[i])
              for i, (a, b) in enumerate(((gg, gg_out), (ug, ug_out), (dg, dg_out)))]
    for c in copies:
        c.start()
    staged[...] = dx[...].reshape(staged.shape)
    copies.append(pltpu.make_async_copy(staged, dx_out, sem.at[3]))
    copies[3].start()
    for c in copies:
        c.wait()


def solution(mesh):
    nz = mesh.shape["seq"] // 2
    nx = mesh.shape["tp"] // 4
    chips = mesh.shape["tp"] // 2

    def per_device(inputs, out_grad, gate_weight, up_weight, down_weight):
        groups, local, depth = inputs.shape
        rows = groups * local
        units = gate_weight.shape[1]
        tokens = rows * mesh.shape["seq"]
        half, share = tokens // 2, tokens // (2 * chips)
        whole = pl.BlockSpec(memory_space=pltpu.VMEM)
        hbm = pl.BlockSpec(memory_space=pltpu.HBM)
        dma = pltpu.SemaphoreType.DMA
        vmem = pltpu.VMEM
        out = pl.pallas_call(
            lambda *refs: kernel(nz, nx, *refs),
            out_shape=(
                vmem((rows, depth), BF16),
                vmem((units, depth), F32), vmem((units, depth), F32), vmem((units, depth), F32),
            ),
            in_specs=[hbm] * 5,
            out_specs=(whole,) * 4,
            scratch_shapes=[
                vmem((groups, local, depth), BF16), vmem((groups, local, depth), BF16),
                vmem((2 * nz, 2, rows, depth), BF16), vmem((4, 2, rows, depth), BF16),
                vmem((units, depth), BF16), vmem((units, depth), BF16), vmem((units, depth), BF16),
                vmem((tokens, depth), BF16), vmem((tokens, depth), BF16),
                vmem((3, half, units), F32), vmem((3, half, units), F32),
                vmem((3, half, units), F32),
                vmem((3, chips, share, units), BF16),
                vmem((chips - 1, 3, share, units), BF16),
                vmem((2 * chips, 3, share, units), BF16),
                vmem((2 * nz, rows, depth), F32),
                vmem((2 * nz, rows, depth), BF16), vmem((len(LEAF_KEYS), rows, depth), BF16),
                vmem((len(INNER_KEYS), rows, depth), F32), vmem((len(INNER_KEYS), rows, depth), F32),
                dma((5,)),
                dma((len(EDGES),)), dma((len(HELD),)), dma((4,)),
                dma((3,)), dma((3,)),
                dma((7, 3)), dma((7, 3)), dma((7,)), dma((7,)), dma((8,)), dma((8,)),
                dma((len(LEAF_KEYS),)), dma((len(LEAF_KEYS),)),
                dma((len(INNER_KEYS),)), dma((len(INNER_KEYS),)),
            ],
            compiler_params=pltpu.CompilerParams(
                collective_id=0, has_side_effects=True, vmem_limit_bytes=48 * 2**20),
        )(*[pltpu.with_memory_space_constraint(a, pltpu.HBM) for a in (
            inputs, out_grad, gate_weight.T, up_weight.T, down_weight)])
        grad = jax.ShapeDtypeStruct((units, depth), F32)
        dx, gg, ug, dg = pl.pallas_call(
            write_out,
            out_shape=(jax.ShapeDtypeStruct((groups, local, depth), BF16), grad, grad, grad),
            in_specs=[whole] * 4,
            out_specs=(hbm,) * 4,
            scratch_shapes=[vmem((groups, local, depth), BF16), dma((4,))],
            compiler_params=pltpu.CompilerParams(vmem_limit_bytes=8 * 2**20),
        )(*out)
        return dx, gg.T, ug.T, dg

    return jax.shard_map(
        per_device, mesh=mesh,
        in_specs=(P(None, "seq", "tp"), P(None, "seq", "tp"), P("tp", "seq"), P("tp", "seq"),
                  P("seq", "tp")),
        out_specs=(P(None, "seq", "tp"), P("tp", "seq"), P("tp", "seq"), P("seq", "tp")),
        check_vma=False)
```

```python
import functools

import jax
import jax.numpy as jnp
from jax import lax
from jax.experimental import pallas as pl
from jax.experimental.pallas import tpu as pltpu
from jax.sharding import PartitionSpec as P

MESH = pl.DeviceIdType.MESH
F32, BF16 = jnp.float32, jnp.bfloat16

FAR_Y = (0, 1, "M")


def onward(core, oz):
    far = "M" if core else "R"
    here = () if core else ((0, 0, "M"),)
    sign = 1 if oz > 0 else -1
    near = ((1, 0, "M"), (-1, 0, "M"))
    if oz == 0:
        return ((3, 0, far), (-3, 0, far)) + near + (FAR_Y,)
    if abs(oz) == 3:
        return ((3 * sign, 0, far),) + near + here + (FAR_Y,)
    if abs(oz) == 6:
        return ((2 * sign, 1, "M"), (2 * sign, 0, "M"), (1, 1, "M"), (-1, 1, "M")) + near + here + (FAR_Y,)
    return (FAR_Y,) if abs(oz) in (1, 2, 4) else ()


def carrier(core, oz):
    return 1 if core or abs(oz) in (3, 6) else 0


INNER = (0, 1, -1, 3, -3, 2, -2, 4, -4, 6, -6)
EDGES = [(core, oz, dz, dy, kind) for core in (1, 0) for oz in INNER for dz, dy, kind in onward(core, oz)]


def inward(core, oz):
    far = "M" if core else "R"
    edges = tuple(e for e in onward(core, oz) if abs(oz) != 3 or abs(e[0]) != 3)
    return edges + (((6, 0, far), (-6, 0, far)) if oz == 0 else ())


UP = {(core, oz + dz, dy, kind): (oz, dz, dy)
      for core in (1, 0) for oz in INNER for dz, dy, kind in inward(core, oz)}


def is_inner(core, oz, dy, kind):
    return dy == 0 and oz in INNER and (kind == "R" or carrier(core, oz) == core)


LEAF_KEYS = [k for k in UP if not is_inner(*k)]
INNER_KEYS = [k for k in UP if is_inner(*k)]
HELD = [k for k in dict.fromkeys((oz + dz, dy) for _, oz, dz, dy, kind in EDGES if kind == "M")]
RELAYED = [3, -3, 6, -6]


def kernel(nz, nx, x_any, dy_any, wg_any, wu_any, wd_any, dx_ref, gg, ug, dg,
           xin, dyin, buf, relay, wg, wu, wd, xs, ys, own, far, got, slabs, landed, act,
           dxp, leaves, lrecv, zsend, zrecv,
           ready, load_sem, zs_sem, zr_sem, rr_sem, cs_sem, cr_sem,
           ts_sem, tr_sem, as_sem, ar_sem, bs_sem, br_sem, fys_sem, fyr_sem, fzs_sem, fzr_sem):
    s = lax.axis_index("seq")
    t = lax.axis_index("tp")
    z, yl = s // 2, s % 2
    core, yh, x = t % 2, (t // 2) % 2, t // 4

    along = {(d, f): lax.rem(z + d + nz, nz) * 2 + (1 - yl if f else yl) for d in range(-8, 9) for f in (0, 1)}
    def seq_at(dz, flip=0):
        return along[dz, flip]

    def chip_at(dx, dyh):
        return lax.rem(x + dx + nx, nx) * 2 + lax.rem(yh + dyh, 2)

    others = [(2, 1), (1, 1), (3, 1), (2, 0), (0, 1), (1, 0), (3, 0)]

    def copy_to(src, dst, send, recv, device):
        return pltpu.make_async_remote_copy(
            src_ref=src, dst_ref=dst, send_sem=send, recv_sem=recv, device_id=device,
            device_id_type=MESH)

    mate = (s, t + 1 - 2 * core)
    across = (seq_at(0, 1), t)
    barrier = pltpu.get_barrier_semaphore()
    on_core = (t - core, t - core + 1)

    def met_by(c):
        met = {(0, 0, 1 - c)}
        for owner, oz, dz, dy, kind in EDGES:
            a, b = carrier(owner, oz), 1 if kind == "R" else owner
            met |= {(dz, dy, b)} if a == c else set()
            met |= {(-dz, dy, a)} if b == c else set()
        return sorted(met - {(0, 0, c)}, key=lambda m: (-abs(m[0]), m))

    def greet(c):
        partners = [(along[d, f], on_core[k]) for d, f, k in met_by(c)]
        partners += [(s, chips_at[others.index(k)] * 2 + core) for k in close]
        for device in partners:
            pl.semaphore_signal(barrier, inc=1, device_id=device, device_id_type=MESH)

    def greeted(c):
        pl.semaphore_wait(barrier, len(met_by(c)) + len(close))
        for device in [(s, chips_at[others.index((0, 1))] * 2 + core)] + [(along[d, 0], t) for d in (3, -3) if c]:
            pl.semaphore_signal(ready, inc=1, device_id=device, device_id_type=MESH)

    def all_ready(c):
        pl.semaphore_wait(ready, 3 if c else 1)

    def on_cores(body):
        for c in (1, 0):
            pl.when(core == c)(functools.partial(body, c))

    chips_at = [chip_at(*k) for k in others]
    close = [(2, 0), (0, 1), (1, 0), (3, 0)]
    loads = [pltpu.make_async_copy(a, b, load_sem.at[i])
             for i, (a, b) in enumerate(((x_any, xin), (dy_any, dyin), (wg_any, wg), (wu_any, wu), (wd_any, wd)))]
    for c in loads[:2]:
        c.start()
    on_cores(greet)
    rows, depth = buf.shape[2], buf.shape[3]
    for c in loads[:2]:
        c.wait()
    buf[s, 0] = xin[...].reshape(rows, depth)
    buf[s, 1] = dyin[...].reshape(rows, depth)
    for c in loads[2:]:
        c.start()
    on_cores(greeted)

    sent = []

    def done():
        for c in sent:
            c.wait_send()
        for k in (0, 1):
            @pl.when(core == k)
            def _(k=k):
                for make in later[k]:
                    make().wait_send()

    def send(*a):
        c = copy_to(*a)
        c.start()
        sent.append(c)

    later = {0: [], 1: []}

    def tp_of(c):
        return on_core[c]

    def issue(c, make):
        make().start()
        later[c].append(make)

    def half_of(ref, oz):
        return ref.at[0] if oz == 8 else ref.at[1] if oz == -8 else ref

    def held(oz, dy):
        return half_of(buf.at[seq_at(-oz, dy)], oz)

    def pass_on(c, oz, kind, by):
        for dz, dy, to in onward(c, oz):
            n = EDGES.index((c, oz, dz, dy, to))
            far = oz + dz

            def make(dz=dz, dy=dy, to=to, n=n, far=far):
                src = relay.at[RELAYED.index(oz)] if kind == "R" else buf.at[seq_at(-oz)]
                dst = relay.at[RELAYED.index(far)] if to == "R" else buf.at[seq_at(-oz)]
                sem = rr_sem.at[RELAYED.index(far)] if to == "R" else zr_sem.at[HELD.index((far, dy))]
                return copy_to(half_of(src, far), half_of(dst, far), zs_sem.at[n], sem,
                               (seq_at(dz, dy), tp_of(1 if to == "R" else c)))
            issue(by, make)

    def arrived(oz, dy):
        ref = held(oz, dy)
        copy_to(ref, ref, zs_sem.at[0], zr_sem.at[HELD.index((oz, dy))], across).wait_recv()

    def relay_arrived(oz):
        i = RELAYED.index(oz)
        copy_to(relay.at[i], relay.at[i], zs_sem.at[0], rr_sem.at[i], across).wait_recv()

    @pl.when(core == 1)
    def _():
        pass_on(1, 0, "M", 1)
        for oz in (1, -1):
            arrived(oz, 0)
            pass_on(1, oz, "M", 1)
        for oz in (3, -3):
            arrived(oz, 0)
            pass_on(1, oz, "M", 1)
        for oz in (3, -3):
            relay_arrived(oz)
            pass_on(0, oz, "R", 1)
        for oz in (2, -2, 4, -4):
            arrived(oz, 0)
            pass_on(1, oz, "M", 1)
        for oz in (6, -6):
            arrived(oz, 0)
            pass_on(1, oz, "M", 1)
        for oz in (6, -6):
            relay_arrived(oz)
            pass_on(0, oz, "R", 1)
        for oz, dy in HELD:
            if dy or oz not in INNER:
                arrived(oz, dy)

    @pl.when(core == 0)
    def _():
        pass_on(0, 0, "M", 0)
        for oz in (1, -1, 2, -2, 4, -4):
            arrived(oz, 0)
            pass_on(0, oz, "M", 0)
        for oz, dy in HELD:
            if dy or oz not in (0, 1, -1, 2, -2, 4, -4):
                arrived(oz, dy)

    xs[...] = buf[:, 0].astype(F32).reshape(xs.shape).astype(BF16)
    ys[...] = buf[:, 1].astype(F32).reshape(ys.shape).astype(BF16)
    for c in loads[2:]:
        c.wait()

    half = xs.shape[0] // 2
    mine = pl.ds(pl.multiple_of(core * half, half), half)
    theirs = pl.ds(pl.multiple_of((1 - core) * half, half), half)
    last = (((1,), (1,)), ((), ()))

    def product(k, at):
        rows_of, weight = ((xs, wg), (xs, wu), (ys, wd))[k]
        return lax.dot_general(rows_of[at, :], weight[...], last, preferred_element_type=F32)

    chips = slabs.shape[1]
    share = half // chips
    on_cores(all_ready)
    for k in range(3):
        far[k] = product(k, theirs)
        send(far.at[k], got.at[k], cs_sem.at[k], cr_sem.at[k], mate)
    own[0] = product(0, mine)
    for k in range(3):
        copy_to(far.at[k], got.at[k], cs_sem.at[k], cr_sem.at[k], mate).wait_recv()
        total = own[k] + got[k]
        own[k] = total
        slabs[k] = total.reshape(chips, share, -1).astype(BF16)
        for i, (a, b) in enumerate(others):
            chip = chip_at(a, b)
            send(slabs.at[k, chip], landed.at[i, k], ts_sem.at[i, k], tr_sem.at[i, k],
                 (s, chip * 2 + core))
        if k < 2:
            own[k + 1] = product(k + 1, mine)
    me = chip_at(0, 0)
    at = core * chips + me
    sums = []
    for k in range(3):
        total = own[k, pl.ds(pl.multiple_of(me * share, share), share), :]
        for i in range(len(others)):
            copy_to(slabs.at[k, 0], landed.at[i, k], ts_sem.at[i, k], tr_sem.at[i, k], mate).wait_recv()
            total = total + landed[i, k].astype(F32)
        sums.append(total)
        if k == 1:
            gate, up = sums
            sig = jax.nn.sigmoid(gate)
            act[at, 0] = (gate * sig * up).astype(BF16)
    grad = sums[2]
    act[at, 1] = (grad * gate * sig).astype(BF16)
    act[at, 2] = (grad * up * sig * (1.0 + gate * (1.0 - sig))).astype(BF16)

    def units_of(g, late):
        return act.at[g, 0] if late else act.at[g, pl.ds(1, 2)]

    def give_units(late):
        ref = units_of(at, late)
        for i, chip in enumerate(chips_at):
            send(ref, ref, as_sem.at[i, late], ar_sem.at[i, late], (s, chip * 2 + core))
        send(ref, ref, bs_sem.at[7, late], br_sem.at[7, late], mate)

    from_chips = [chip_at(-a, b) for a, b in others] + [me]

    def hand_over_units(late):
        for i in range(len(others)):
            ref = units_of(core * chips + from_chips[i], late)
            copy_to(ref, ref, as_sem.at[i, late], ar_sem.at[i, late], mate).wait_recv()
            send(ref, ref, bs_sem.at[i, late], br_sem.at[i, late], mate)

    def units_complete(late):
        for i, chip in enumerate(from_chips):
            ref = units_of((1 - core) * chips + chip, late)
            copy_to(ref, ref, bs_sem.at[i, late], br_sem.at[i, late], mate).wait_recv()

    give_units(0)
    give_units(1)
    hand_over_units(0)
    units_complete(0)

    tokens, units = xs.shape[0], wg.shape[0]
    gate_unit = act[:, 2].reshape(tokens, units)
    up_unit = act[:, 1].reshape(tokens, units)
    term = jnp.dot(gate_unit, wg[...], preferred_element_type=F32)
    term = term + jnp.dot(up_unit, wu[...], preferred_element_type=F32)
    dxp[...] = term.reshape(dxp.shape)

    leaves[...] = term.reshape(dxp.shape).astype(BF16)
    first = (((0,), (0,)), ((), ()))
    wide = depth // 2

    def side(ref, oz):
        return ref.at[:, pl.ds(0, wide)] if oz == 8 else ref.at[:, pl.ds(wide, wide)] if oz == -8 else ref

    def send_up(key, by):
        c, oz, dy, kind = key
        up, dz, _ = UP[key]
        target = (seq_at(-dz, dy), tp_of(carrier(c, up)))
        if key in INNER_KEYS:
            n = INNER_KEYS.index(key)
            issue(by, lambda: copy_to(zsend.at[n], zrecv.at[n], fzs_sem.at[n], fzr_sem.at[n], target))
        else:
            n = LEAF_KEYS.index(key)
            issue(by, lambda: copy_to(side(leaves.at[seq_at(-oz, dy)], oz), side(lrecv.at[n], oz),
                                      fys_sem.at[n], fyr_sem.at[n], target))

    def collected(c, oz):
        kind = "R" if carrier(c, oz) != c else "M"
        value = jnp.zeros((rows, depth), F32) if kind == "R" else dxp[seq_at(-oz)]
        for dz, dy, to in inward(c, oz):
            key = (c, oz + dz, dy, to)
            if key in INNER_KEYS:
                n = INNER_KEYS.index(key)
                copy_to(zsend.at[n], zrecv.at[n], fzs_sem.at[n], fzr_sem.at[n], across).wait_recv()
                value = value + zrecv[n]
            else:
                n = LEAF_KEYS.index(key)
                ref = side(lrecv.at[n], key[1])
                copy_to(ref, ref, fys_sem.at[n], fyr_sem.at[n], across).wait_recv()
                nothing = jnp.zeros((rows, wide), F32)
                if key[1] == 8:
                    value = value + jnp.concatenate([lrecv[n, :, :wide].astype(F32), nothing], axis=1)
                elif key[1] == -8:
                    value = value + jnp.concatenate([nothing, lrecv[n, :, wide:].astype(F32)], axis=1)
                else:
                    value = value + lrecv[n].astype(F32)
        return value

    def forward(c, oz, by):
        key = (c, oz, 0, "R" if carrier(c, oz) != c else "M")
        zsend[INNER_KEYS.index(key)] = collected(c, oz)
        send_up(key, by)

    urgent = (8, 7, 5, 6, 4, 2, 3, 1, 0)

    def start_leaves(c):
        mine = [k for k in LEAF_KEYS if k[0] == c]
        for key in sorted(mine, key=lambda k: (urgent.index(abs(k[1])), -k[2])):
            send_up(key, c)

    def middle(c):
        for oz in (4, -4, 2, -2, 1, -1):
            forward(c, oz, c)

    def outer(c):
        for oz in (6, -6):
            for b in ((1, 0) if c else ()):
                forward(b, oz, c)

    def finish(c):
        for oz in (3, -3):
            for b in ((1, 0) if c else ()):
                forward(b, oz, c)
        dx_ref[...] = collected(c, 0).astype(BF16)

    on_cores(start_leaves)
    hand_over_units(1)
    gg[...] = lax.dot_general(gate_unit, xs[...], first, preferred_element_type=F32)
    on_cores(middle)
    on_cores(outer)
    ug[...] = lax.dot_general(up_unit, xs[...], first, preferred_element_type=F32)
    units_complete(1)
    dg[...] = lax.dot_general(act[:, 0].reshape(tokens, units), ys[...], first,
                              preferred_element_type=F32)
    on_cores(finish)

    done()


def write_out(dx, gg, ug, dg, dx_out, gg_out, ug_out, dg_out, staged, sem):
    copies = [pltpu.make_async_copy(a, b, sem.at[i])
              for i, (a, b) in enumerate(((gg, gg_out), (ug, ug_out), (dg, dg_out)))]
    for c in copies:
        c.start()
    staged[...] = dx[...].reshape(staged.shape)
    copies.append(pltpu.make_async_copy(staged, dx_out, sem.at[3]))
    copies[3].start()
    for c in copies:
        c.wait()


def solution(mesh):
    nz = mesh.shape["seq"] // 2
    nx = mesh.shape["tp"] // 4
    chips = mesh.shape["tp"] // 2

    def per_device(inputs, out_grad, gate_weight, up_weight, down_weight):
        groups, local, depth = inputs.shape
        rows = groups * local
        units = gate_weight.shape[1]
        tokens = rows * mesh.shape["seq"]
        half, share = tokens // 2, tokens // (2 * chips)
        whole = pl.BlockSpec(memory_space=pltpu.VMEM)
        hbm = pl.BlockSpec(memory_space=pltpu.HBM)
        dma = pltpu.SemaphoreType.DMA
        vmem = pltpu.VMEM
        out = pl.pallas_call(
            lambda *refs: kernel(nz, nx, *refs),
            out_shape=(
                vmem((rows, depth), BF16),
                vmem((units, depth), F32), vmem((units, depth), F32), vmem((units, depth), F32),
            ),
            in_specs=[hbm] * 5,
            out_specs=(whole,) * 4,
            scratch_shapes=[
                vmem((groups, local, depth), BF16), vmem((groups, local, depth), BF16),
                vmem((2 * nz, 2, rows, depth), BF16), vmem((4, 2, rows, depth), BF16),
                vmem((units, depth), BF16), vmem((units, depth), BF16), vmem((units, depth), BF16),
                vmem((tokens, depth), BF16), vmem((tokens, depth), BF16),
                vmem((3, half, units), F32), vmem((3, half, units), F32),
                vmem((3, half, units), F32),
                vmem((3, chips, share, units), BF16),
                vmem((chips - 1, 3, share, units), BF16),
                vmem((2 * chips, 3, share, units), BF16),
                vmem((2 * nz, rows, depth), F32),
                vmem((2 * nz, rows, depth), BF16), vmem((len(LEAF_KEYS), rows, depth), BF16),
                vmem((len(INNER_KEYS), rows, depth), F32), vmem((len(INNER_KEYS), rows, depth), F32),
                pltpu.SemaphoreType.REGULAR, dma((5,)),
                dma((len(EDGES),)), dma((len(HELD),)), dma((4,)),
                dma((3,)), dma((3,)),
                dma((7, 3)), dma((7, 3)), dma((7, 2)), dma((7, 2)), dma((8, 2)), dma((8, 2)),
                dma((len(LEAF_KEYS),)), dma((len(LEAF_KEYS),)),
                dma((len(INNER_KEYS),)), dma((len(INNER_KEYS),)),
            ],
            compiler_params=pltpu.CompilerParams(
                collective_id=0, has_side_effects=True, vmem_limit_bytes=48 * 2**20),
        )(*[pltpu.with_memory_space_constraint(a, pltpu.HBM) for a in (
            inputs, out_grad, gate_weight.T, up_weight.T, down_weight)])
        grad = jax.ShapeDtypeStruct((units, depth), F32)
        dx, gg, ug, dg = pl.pallas_call(
            write_out,
            out_shape=(jax.ShapeDtypeStruct((groups, local, depth), BF16), grad, grad, grad),
            in_specs=[whole] * 4,
            out_specs=(hbm,) * 4,
            scratch_shapes=[vmem((groups, local, depth), BF16), dma((4,))],
            compiler_params=pltpu.CompilerParams(vmem_limit_bytes=8 * 2**20),
        )(*out)
        return dx, gg.T, ug.T, dg

    return jax.shard_map(
        per_device, mesh=mesh,
        in_specs=(P(None, "seq", "tp"), P(None, "seq", "tp"), P("tp", "seq"), P("tp", "seq"),
                  P("seq", "tp")),
        out_specs=(P(None, "seq", "tp"), P("tp", "seq"), P("tp", "seq"), P("seq", "tp")),
        check_vma=False)
```

```python
import functools

import jax
import jax.numpy as jnp
from jax import lax
from jax.experimental import pallas as pl
from jax.experimental.pallas import tpu as pltpu
from jax.sharding import PartitionSpec as P

MESH = pl.DeviceIdType.MESH
F32, BF16 = jnp.float32, jnp.bfloat16

FAR_Y = (0, 1, "M")


def onward(core, oz):
    far = "M" if core else "R"
    here = () if core else ((0, 0, "M"),)
    sign = 1 if oz > 0 else -1
    near = ((1, 0, "M"), (-1, 0, "M"))
    if oz == 0:
        return ((3, 0, far), (-3, 0, far)) + near + (FAR_Y,)
    if abs(oz) == 3:
        return ((3 * sign, 0, far),) + near + here + (FAR_Y,)
    if abs(oz) == 6:
        return ((2 * sign, 1, "M"), (2 * sign, 0, "M"), (1, 1, "M"), (-1, 1, "M")) + near + here + (FAR_Y,)
    return (FAR_Y,) if abs(oz) in (1, 2, 4) else ()


def carrier(core, oz):
    return 1 if core or abs(oz) in (3, 6) else 0


INNER = (0, 1, -1, 3, -3, 2, -2, 4, -4, 6, -6)
EDGES = [(core, oz, dz, dy, kind) for core in (1, 0) for oz in INNER for dz, dy, kind in onward(core, oz)]


def inward(core, oz):
    far = "M" if core else "R"
    edges = tuple(e for e in onward(core, oz) if abs(oz) != 3 or abs(e[0]) != 3)
    return edges + (((6, 0, far), (-6, 0, far)) if oz == 0 else ())


UP = {(core, oz + dz, dy, kind): (oz, dz, dy)
      for core in (1, 0) for oz in INNER for dz, dy, kind in inward(core, oz)}


def is_inner(core, oz, dy, kind):
    return dy == 0 and oz in INNER and (kind == "R" or carrier(core, oz) == core)


LEAF_KEYS = [k for k in UP if not is_inner(*k)]
INNER_KEYS = [k for k in UP if is_inner(*k)]
HELD = [k for k in dict.fromkeys((oz + dz, dy) for _, oz, dz, dy, kind in EDGES if kind == "M")]
RELAYED = [3, -3, 6, -6]


def kernel(nz, nx, x_any, dy_any, wg_any, wu_any, wd_any, dx_ref, gg, ug, dg,
           xin, dyin, buf, relay, wg, wu, wd, xs, ys, own, far, got, slabs, landed, act,
           dxp, leaves, lrecv, zsend, zrecv,
           ready, load_sem, zs_sem, zr_sem, rr_sem, cs_sem, cr_sem,
           ts_sem, tr_sem, as_sem, ar_sem, bs_sem, br_sem, fys_sem, fyr_sem, fzs_sem, fzr_sem):
    s = lax.axis_index("seq")
    t = lax.axis_index("tp")
    z, yl = s // 2, s % 2
    core, yh, x = t % 2, (t // 2) % 2, t // 4

    along = {(d, f): lax.rem(z + d + nz, nz) * 2 + (1 - yl if f else yl) for d in range(-8, 9) for f in (0, 1)}
    def seq_at(dz, flip=0):
        return along[dz, flip]

    def chip_at(dx, dyh):
        return lax.rem(x + dx + nx, nx) * 2 + lax.rem(yh + dyh, 2)

    others = [(2, 1), (1, 1), (3, 1), (2, 0), (0, 1), (1, 0), (3, 0)]

    def copy_to(src, dst, send, recv, device):
        return pltpu.make_async_remote_copy(
            src_ref=src, dst_ref=dst, send_sem=send, recv_sem=recv, device_id=device,
            device_id_type=MESH)

    mate = (s, t + 1 - 2 * core)
    across = (seq_at(0, 1), t)
    barrier = pltpu.get_barrier_semaphore()
    on_core = (t - core, t - core + 1)

    def met_by(c):
        met = {(0, 0, 1 - c)}
        for owner, oz, dz, dy, kind in EDGES:
            a, b = carrier(owner, oz), 1 if kind == "R" else owner
            met |= {(dz, dy, b)} if a == c else set()
            met |= {(-dz, dy, a)} if b == c else set()
        return sorted(met - {(0, 0, c)}, key=lambda m: (-abs(m[0]), m))

    def greet(c):
        partners = [(along[d, f], on_core[k]) for d, f, k in met_by(c)]
        partners += [(s, chips_at[others.index(k)] * 2 + core) for k in close]
        for device in partners:
            pl.semaphore_signal(barrier, inc=1, device_id=device, device_id_type=MESH)

    def greeted(c):
        pl.semaphore_wait(barrier, len(met_by(c)) + len(close))
        for device in [(s, chips_at[others.index((0, 1))] * 2 + core)] + [(along[d, 0], t) for d in (3, -3) if c]:
            pl.semaphore_signal(ready, inc=1, device_id=device, device_id_type=MESH)

    def all_ready(c):
        pl.semaphore_wait(ready, 3 if c else 1)

    def on_cores(body):
        for c in (1, 0):
            pl.when(core == c)(functools.partial(body, c))

    chips_at = [chip_at(*k) for k in others]
    close = [(2, 0), (0, 1), (1, 0), (3, 0)]
    loads = [pltpu.make_async_copy(a, b, load_sem.at[i])
             for i, (a, b) in enumerate(((x_any, xin), (dy_any, dyin), (wg_any, wg), (wu_any, wu), (wd_any, wd)))]
    for c in loads[:2]:
        c.start()
    on_cores(greet)
    rows, depth = buf.shape[2], buf.shape[3]
    for c in loads[:2]:
        c.wait()
    buf[s, 0] = xin[...].reshape(rows, depth)
    buf[s, 1] = dyin[...].reshape(rows, depth)
    for c in loads[2:]:
        c.start()
    on_cores(greeted)

    sent = []

    def done():
        for c in sent:
            c.wait_send()
        sent.clear()

        def left(c):
            for make in later[c]:
                make().wait_send()
            later[c].clear()
        on_cores(left)

    def send(*a):
        c = copy_to(*a)
        c.start()
        sent.append(c)

    later = {0: [], 1: []}

    def tp_of(c):
        return on_core[c]

    def issue(c, make):
        make().start()
        later[c].append(make)

    wide = depth // 2

    def side(ref, oz):
        return ref.at[:, pl.ds(0, wide)] if oz == 8 else ref.at[:, pl.ds(wide, wide)] if oz == -8 else ref

    def pass_on(c, oz, j, by):
        relays = carrier(c, oz) != c
        for dz, dy, to in onward(c, oz):
            n = EDGES.index((c, oz, dz, dy, to))
            far = oz + dz

            def make(dz=dz, dy=dy, to=to, n=n, far=far):
                src = relay.at[RELAYED.index(oz), j] if relays else buf.at[seq_at(-oz), j]
                dst = relay.at[RELAYED.index(far), j] if to == "R" else buf.at[seq_at(-oz), j]
                sem = rr_sem.at[RELAYED.index(far), j] if to == "R" else zr_sem.at[HELD.index((far, dy)), j]
                return copy_to(side(src, far), side(dst, far), zs_sem.at[n, j], sem,
                               (seq_at(dz, dy), tp_of(1 if to == "R" else c)))
            issue(by, make)

    def arrived(oz, dy, j):
        ref = side(buf.at[seq_at(-oz, dy), j], oz)
        copy_to(ref, ref, zs_sem.at[0, 0], zr_sem.at[HELD.index((oz, dy)), j], across).wait_recv()

    def relay_arrived(oz, j):
        ref = relay.at[RELAYED.index(oz), j]
        copy_to(ref, ref, zs_sem.at[0, 0], rr_sem.at[RELAYED.index(oz), j], across).wait_recv()

    def relay_blocks(c):
        def stage(j, offsets):
            for owner in ((1, 0) if c else (0,)):
                for oz in offsets:
                    if carrier(owner, oz) != c:
                        continue
                    if owner == c:
                        arrived(oz, 0, j)
                    else:
                        relay_arrived(oz, j)
                    pass_on(owner, oz, j, c)
        for j in (0, 1):
            pass_on(c, 0, j, c)
        stage(0, (3, -3))
        stage(0, (1, -1))
        stage(1, (3, -3))
        stage(1, (1, -1))
        stage(0, (2, -2, 4, -4))
        stage(0, (6, -6))
        stage(1, (2, -2, 4, -4))
        stage(1, (6, -6))
        leaves_complete(c, 0)

    def leaves_complete(c, j):
        for oz, dy in sorted(HELD, key=lambda h: abs(h[0]) + h[1]):
            if dy or oz not in INNER or carrier(c, oz) != c:
                arrived(oz, dy, j)

    on_cores(relay_blocks)
    for c in loads[2:]:
        c.wait()
    xs[...] = buf[:, 0].astype(F32).reshape(xs.shape).astype(BF16)

    half = xs.shape[0] // 2
    mine = pl.ds(pl.multiple_of(core * half, half), half)
    theirs = pl.ds(pl.multiple_of((1 - core) * half, half), half)
    last = (((1,), (1,)), ((), ()))

    def product(k, at):
        rows_of, weight = ((xs, wg), (xs, wu), (ys, wd))[k]
        return lax.dot_general(rows_of[at, :], weight[...], last, preferred_element_type=F32)

    chips = slabs.shape[1]
    share = half // chips
    def to_mate(k):
        far[k] = product(k, theirs)
        send(far.at[k], got.at[k], cs_sem.at[k], cr_sem.at[k], mate)

    on_cores(all_ready)
    to_mate(0)
    to_mate(1)
    own[0] = product(0, mine)
    for k in range(3):
        copy_to(far.at[k], got.at[k], cs_sem.at[k], cr_sem.at[k], mate).wait_recv()
        total = own[k] + got[k]
        own[k] = total
        slabs[k] = total.reshape(chips, share, -1).astype(BF16)
        for i, (a, b) in enumerate(others):
            chip = chip_at(a, b)
            send(slabs.at[k, chip], landed.at[i, k], ts_sem.at[i, k], tr_sem.at[i, k],
                 (s, chip * 2 + core))
        if k == 0:
            own[1] = product(1, mine)
        if k == 1:
            on_cores(lambda c: leaves_complete(c, 1))
            ys[...] = buf[:, 1].astype(F32).reshape(ys.shape).astype(BF16)
            to_mate(2)
            own[2] = product(2, mine)
    done()
    me = chip_at(0, 0)
    at = core * chips + me
    sums = []
    for k in range(3):
        total = own[k, pl.ds(pl.multiple_of(me * share, share), share), :]
        for i in reversed(range(len(others))):
            copy_to(slabs.at[k, 0], landed.at[i, k], ts_sem.at[i, k], tr_sem.at[i, k], mate).wait_recv()
            total = total + landed[i, k].astype(F32)
        sums.append(total)
        if k == 1:
            gate, up = sums
            sig = jax.nn.sigmoid(gate)
            act[at, 0] = (gate * sig * up).astype(BF16)
    grad = sums[2]
    act[at, 1] = (grad * gate * sig).astype(BF16)
    act[at, 2] = (grad * up * sig * (1.0 + gate * (1.0 - sig))).astype(BF16)

    def units_of(g, late):
        return act.at[g, 0] if late else act.at[g, pl.ds(1, 2)]

    def give_units(late):
        ref = units_of(at, late)
        for i, chip in enumerate(chips_at):
            send(ref, ref, as_sem.at[i, late], ar_sem.at[i, late], (s, chip * 2 + core))
        send(ref, ref, bs_sem.at[7, late], br_sem.at[7, late], mate)

    from_chips = [chip_at(-a, b) for a, b in others] + [me]

    def hand_over_units(late):
        for i in reversed(range(len(others))):
            ref = units_of(core * chips + from_chips[i], late)
            copy_to(ref, ref, as_sem.at[i, late], ar_sem.at[i, late], mate).wait_recv()
            send(ref, ref, bs_sem.at[i, late], br_sem.at[i, late], mate)

    def units_complete(late):
        for i, chip in reversed(list(enumerate(from_chips))):
            ref = units_of((1 - core) * chips + chip, late)
            copy_to(ref, ref, bs_sem.at[i, late], br_sem.at[i, late], mate).wait_recv()

    give_units(0)
    give_units(1)
    hand_over_units(0)
    units_complete(0)

    tokens, units = xs.shape[0], wg.shape[0]
    gate_unit = act[:, 2].reshape(tokens, units)
    up_unit = act[:, 1].reshape(tokens, units)
    term = jnp.dot(gate_unit, wg[...], preferred_element_type=F32)
    term = term + jnp.dot(up_unit, wu[...], preferred_element_type=F32)
    dxp[...] = term.reshape(dxp.shape)

    leaves[...] = term.reshape(dxp.shape).astype(BF16)
    first = (((0,), (0,)), ((), ()))
    def send_up(key, by):
        c, oz, dy, kind = key
        up, dz, _ = UP[key]
        target = (seq_at(-dz, dy), tp_of(carrier(c, up)))
        if key in INNER_KEYS:
            n = INNER_KEYS.index(key)
            issue(by, lambda: copy_to(zsend.at[n], zrecv.at[n], fzs_sem.at[n], fzr_sem.at[n], target))
        else:
            n = LEAF_KEYS.index(key)
            issue(by, lambda: copy_to(side(leaves.at[seq_at(-oz, dy)], oz), side(lrecv.at[n], oz),
                                      fys_sem.at[n], fyr_sem.at[n], target))

    def collected(c, oz):
        kind = "R" if carrier(c, oz) != c else "M"
        value = jnp.zeros((rows, depth), F32) if kind == "R" else dxp[seq_at(-oz)]
        edges = inward(c, oz)
        for dz, dy, to in sorted(edges, key=lambda e: abs(e[0])) if oz == 0 else edges[::-1]:
            key = (c, oz + dz, dy, to)
            if key in INNER_KEYS:
                n = INNER_KEYS.index(key)
                copy_to(zsend.at[n], zrecv.at[n], fzs_sem.at[n], fzr_sem.at[n], across).wait_recv()
                value = value + zrecv[n]
            else:
                n = LEAF_KEYS.index(key)
                ref = side(lrecv.at[n], key[1])
                copy_to(ref, ref, fys_sem.at[n], fyr_sem.at[n], across).wait_recv()
                nothing = jnp.zeros((rows, wide), F32)
                if key[1] == 8:
                    value = value + jnp.concatenate([lrecv[n, :, :wide].astype(F32), nothing], axis=1)
                elif key[1] == -8:
                    value = value + jnp.concatenate([nothing, lrecv[n, :, wide:].astype(F32)], axis=1)
                else:
                    value = value + lrecv[n].astype(F32)
        return value

    def forward(c, oz, by):
        key = (c, oz, 0, "R" if carrier(c, oz) != c else "M")
        zsend[INNER_KEYS.index(key)] = collected(c, oz)
        send_up(key, by)

    urgent = (8, 7, 5, 6, 4, 2, 3, 1, 0)

    def start_leaves(c):
        mine = [k for k in LEAF_KEYS if k[0] == c]
        for key in sorted(mine, key=lambda k: (urgent.index(abs(k[1])), -k[2])):
            send_up(key, c)

    def middle(c):
        for oz in (4, -4, 2, -2):
            forward(c, oz, c)

    def inner(c):
        for oz in (1, -1):
            forward(c, oz, c)

    def outer(c):
        for b in ((1, 0) if c else ()):
            for oz in (6, -6):
                forward(b, oz, c)

    def three(c):
        for b in ((1, 0) if c else ()):
            for oz in (3, -3):
                forward(b, oz, c)

    def finish(c):
        dx_ref[...] = collected(c, 0).astype(BF16)

    on_cores(start_leaves)
    on_cores(outer)
    on_cores(middle)
    on_cores(inner)
    hand_over_units(1)
    gg[...] = lax.dot_general(gate_unit, xs[...], first, preferred_element_type=F32)
    ug[...] = lax.dot_general(up_unit, xs[...], first, preferred_element_type=F32)
    units_complete(1)
    dg[...] = lax.dot_general(act[:, 0].reshape(tokens, units), ys[...], first,
                              preferred_element_type=F32)
    on_cores(three)
    done()
    on_cores(finish)


def write_out(dx, gg, ug, dg, dx_out, gg_out, ug_out, dg_out, staged, sem):
    copies = [pltpu.make_async_copy(a, b, sem.at[i])
              for i, (a, b) in enumerate(((gg, gg_out), (ug, ug_out), (dg, dg_out)))]
    for c in copies:
        c.start()
    staged[...] = dx[...].reshape(staged.shape)
    copies.append(pltpu.make_async_copy(staged, dx_out, sem.at[3]))
    copies[3].start()
    for c in copies:
        c.wait()


def solution(mesh):
    nz = mesh.shape["seq"] // 2
    nx = mesh.shape["tp"] // 4
    chips = mesh.shape["tp"] // 2

    def per_device(inputs, out_grad, gate_weight, up_weight, down_weight):
        groups, local, depth = inputs.shape
        rows = groups * local
        units = gate_weight.shape[1]
        tokens = rows * mesh.shape["seq"]
        half, share = tokens // 2, tokens // (2 * chips)
        whole = pl.BlockSpec(memory_space=pltpu.VMEM)
        hbm = pl.BlockSpec(memory_space=pltpu.HBM)
        dma = pltpu.SemaphoreType.DMA
        vmem = pltpu.VMEM
        out = pl.pallas_call(
            lambda *refs: kernel(nz, nx, *refs),
            out_shape=(
                vmem((rows, depth), BF16),
                vmem((units, depth), F32), vmem((units, depth), F32), vmem((units, depth), F32),
            ),
            in_specs=[hbm] * 5,
            out_specs=(whole,) * 4,
            scratch_shapes=[
                vmem((groups, local, depth), BF16), vmem((groups, local, depth), BF16),
                vmem((2 * nz, 2, rows, depth), BF16), vmem((4, 2, rows, depth), BF16),
                vmem((units, depth), BF16), vmem((units, depth), BF16), vmem((units, depth), BF16),
                vmem((tokens, depth), BF16), vmem((tokens, depth), BF16),
                vmem((3, half, units), F32), vmem((3, half, units), F32),
                vmem((3, half, units), F32),
                vmem((3, chips, share, units), BF16),
                vmem((chips - 1, 3, share, units), BF16),
                vmem((2 * chips, 3, share, units), BF16),
                vmem((2 * nz, rows, depth), F32),
                vmem((2 * nz, rows, depth), BF16), vmem((len(LEAF_KEYS), rows, depth), BF16),
                vmem((len(INNER_KEYS), rows, depth), F32), vmem((len(INNER_KEYS), rows, depth), F32),
                pltpu.SemaphoreType.REGULAR, dma((5,)),
                dma((len(EDGES), 2)), dma((len(HELD), 2)), dma((4, 2)),
                dma((3,)), dma((3,)),
                dma((7, 3)), dma((7, 3)), dma((7, 2)), dma((7, 2)), dma((8, 2)), dma((8, 2)),
                dma((len(LEAF_KEYS),)), dma((len(LEAF_KEYS),)),
                dma((len(INNER_KEYS),)), dma((len(INNER_KEYS),)),
            ],
            compiler_params=pltpu.CompilerParams(
                collective_id=0, has_side_effects=True, vmem_limit_bytes=48 * 2**20),
        )(*[pltpu.with_memory_space_constraint(a, pltpu.HBM) for a in (
            inputs, out_grad, gate_weight.T, up_weight.T, down_weight)])
        grad = jax.ShapeDtypeStruct((units, depth), F32)
        dx, gg, ug, dg = pl.pallas_call(
            write_out,
            out_shape=(jax.ShapeDtypeStruct((groups, local, depth), BF16), grad, grad, grad),
            in_specs=[whole] * 4,
            out_specs=(hbm,) * 4,
            scratch_shapes=[vmem((groups, local, depth), BF16), dma((4,))],
            compiler_params=pltpu.CompilerParams(vmem_limit_bytes=8 * 2**20),
        )(*out)
        return dx, gg.T, ug.T, dg

    return jax.shard_map(
        per_device, mesh=mesh,
        in_specs=(P(None, "seq", "tp"), P(None, "seq", "tp"), P("tp", "seq"), P("tp", "seq"),
                  P("seq", "tp")),
        out_specs=(P(None, "seq", "tp"), P("tp", "seq"), P("tp", "seq"), P("seq", "tp")),
        check_vma=False)
```

```python
import functools

import jax
import jax.numpy as jnp
from jax import lax
from jax.experimental import pallas as pl
from jax.experimental.pallas import tpu as pltpu
from jax.sharding import PartitionSpec as P

MESH = pl.DeviceIdType.MESH
F32, BF16 = jnp.float32, jnp.bfloat16

FAR_Y = (0, 1, "M")


def onward(core, oz):
    far = "M" if core else "R"
    here = () if core else ((0, 0, "M"),)
    sign = 1 if oz > 0 else -1
    near = ((1, 0, "M"), (-1, 0, "M"))
    if oz == 0:
        return ((3, 0, far), (-3, 0, far)) + near + (FAR_Y,)
    if abs(oz) == 3:
        return ((3 * sign, 0, far),) + near + here + (FAR_Y,)
    if abs(oz) == 6:
        return ((2 * sign, 1, "M"), (2 * sign, 0, "M"), (1, 1, "M"), (-1, 1, "M")) + near + here + (FAR_Y,)
    return (FAR_Y,) if abs(oz) in (1, 2, 4) else ()


def carrier(core, oz):
    return 1 if core or abs(oz) in (3, 6) else 0


INNER = (0, 1, -1, 3, -3, 2, -2, 4, -4, 6, -6)
EDGES = [(core, oz, dz, dy, kind) for core in (1, 0) for oz in INNER for dz, dy, kind in onward(core, oz)]


def inward(core, oz):
    far = "M" if core else "R"
    edges = tuple(e for e in onward(core, oz) if abs(oz) != 3 or abs(e[0]) != 3)
    return edges + (((6, 0, far), (-6, 0, far)) if oz == 0 else ())


UP = {(core, oz + dz, dy, kind): (oz, dz, dy)
      for core in (1, 0) for oz in INNER for dz, dy, kind in inward(core, oz)}


def is_inner(core, oz, dy, kind):
    return dy == 0 and oz in INNER and (kind == "R" or carrier(core, oz) == core)


LEAF_KEYS = [k for k in UP if not is_inner(*k)]
INNER_KEYS = [k for k in UP if is_inner(*k)]
HELD = [k for k in dict.fromkeys((oz + dz, dy) for _, oz, dz, dy, kind in EDGES if kind == "M")]
RELAYED = [3, -3, 6, -6]


def kernel(nz, nx, x_any, dy_any, wg_any, wu_any, wd_any, dx_ref, gg, ug, dg,
           xin, dyin, buf, relay, wg, wu, wd, xs, ys, own, far, got, slabs, landed, act,
           dxp, leaves, lrecv, zsend, zrecv,
           ready, load_sem, zs_sem, zr_sem, rr_sem, cs_sem, cr_sem,
           ts_sem, tr_sem, as_sem, ar_sem, bs_sem, br_sem, fys_sem, fyr_sem, fzs_sem, fzr_sem):
    s = lax.axis_index("seq")
    t = lax.axis_index("tp")
    z, yl = s // 2, s % 2
    core, yh, x = t % 2, (t // 2) % 2, t // 4

    along = {(d, f): lax.rem(z + d + nz, nz) * 2 + (1 - yl if f else yl) for d in range(-8, 9) for f in (0, 1)}
    def seq_at(dz, flip=0):
        return along[dz, flip]

    def chip_at(dx, dyh):
        return lax.rem(x + dx + nx, nx) * 2 + lax.rem(yh + dyh, 2)

    others = [(2, 1), (1, 1), (3, 1), (2, 0), (0, 1), (1, 0), (3, 0)]

    def copy_to(src, dst, send, recv, device):
        return pltpu.make_async_remote_copy(
            src_ref=src, dst_ref=dst, send_sem=send, recv_sem=recv, device_id=device,
            device_id_type=MESH)

    mate = (s, t + 1 - 2 * core)
    across = (seq_at(0, 1), t)
    barrier = pltpu.get_barrier_semaphore()
    on_core = (t - core, t - core + 1)

    def met_by(c):
        met = {(0, 0, 1 - c)}
        for owner, oz, dz, dy, kind in EDGES:
            a, b = carrier(owner, oz), 1 if kind == "R" else owner
            met |= {(dz, dy, b)} if a == c else set()
            met |= {(-dz, dy, a)} if b == c else set()
        return sorted(met - {(0, 0, c)}, key=lambda m: (-abs(m[0]), m))

    def greet(c):
        partners = [(along[d, f], on_core[k]) for d, f, k in met_by(c)]
        partners += [(s, chips_at[others.index(k)] * 2 + core) for k in close]
        for device in partners:
            pl.semaphore_signal(barrier, inc=1, device_id=device, device_id_type=MESH)

    def greeted(c):
        pl.semaphore_wait(barrier, len(met_by(c)) + len(close))
        for device in [(s, chips_at[others.index((0, 1))] * 2 + core)] + [(along[d, 0], t) for d in (3, -3) if c]:
            pl.semaphore_signal(ready, inc=1, device_id=device, device_id_type=MESH)

    def all_ready(c):
        pl.semaphore_wait(ready, 3 if c else 1)

    def on_cores(body):
        for c in (1, 0):
            pl.when(core == c)(functools.partial(body, c))

    chips_at = [chip_at(*k) for k in others]
    close = [(2, 0), (0, 1), (1, 0), (3, 0)]
    loads = [pltpu.make_async_copy(a, b, load_sem.at[i])
             for i, (a, b) in enumerate(((x_any, xin), (dy_any, dyin), (wg_any, wg), (wu_any, wu), (wd_any, wd)))]
    for c in loads[:2]:
        c.start()
    on_cores(greet)
    rows, depth = buf.shape[2], buf.shape[3]
    for c in loads[:2]:
        c.wait()
    buf[s, 0] = xin[...].reshape(rows, depth)
    buf[s, 1] = dyin[...].reshape(rows, depth)
    for c in loads[2:]:
        c.start()
    on_cores(greeted)

    sent = []

    def done():
        for c in sent:
            c.wait_send()
        sent.clear()

        def left(c):
            for make in later[c]:
                make().wait_send()
            later[c].clear()
        on_cores(left)

    def send(*a):
        c = copy_to(*a)
        c.start()
        sent.append(c)

    later = {0: [], 1: []}

    def tp_of(c):
        return on_core[c]

    def issue(c, make):
        make().start()
        later[c].append(make)

    wide = depth // 2

    def side(ref, oz):
        return ref.at[:, pl.ds(0, wide)] if oz == 8 else ref.at[:, pl.ds(wide, wide)] if oz == -8 else ref

    def pass_on(c, oz, j, by, lengths=(0, 1, 2, 3)):
        relays = carrier(c, oz) != c
        for dz, dy, to in onward(c, oz):
            if abs(dz) not in lengths:
                continue
            n = EDGES.index((c, oz, dz, dy, to))
            far = oz + dz

            def make(dz=dz, dy=dy, to=to, n=n, far=far):
                src = relay.at[RELAYED.index(oz), j] if relays else buf.at[seq_at(-oz), j]
                dst = relay.at[RELAYED.index(far), j] if to == "R" else buf.at[seq_at(-oz), j]
                sem = rr_sem.at[RELAYED.index(far), j] if to == "R" else zr_sem.at[HELD.index((far, dy)), j]
                return copy_to(side(src, far), side(dst, far), zs_sem.at[n, j], sem,
                               (seq_at(dz, dy), tp_of(1 if to == "R" else c)))
            issue(by, make)

    def arrived(oz, dy, j):
        ref = side(buf.at[seq_at(-oz, dy), j], oz)
        copy_to(ref, ref, zs_sem.at[0, 0], zr_sem.at[HELD.index((oz, dy)), j], across).wait_recv()

    def relay_arrived(oz, j):
        ref = relay.at[RELAYED.index(oz), j]
        copy_to(ref, ref, zs_sem.at[0, 0], rr_sem.at[RELAYED.index(oz), j], across).wait_recv()

    def relay_blocks(c):
        def stage(j, offsets):
            here = [(owner, oz) for owner in ((1, 0) if c else (0,)) for oz in offsets
                    if carrier(owner, oz) == c]
            for owner, oz in here:
                if owner == c:
                    arrived(oz, 0, j)
                else:
                    relay_arrived(oz, j)
                pass_on(owner, oz, j, c, (3,) if abs(oz) == 3 else (0, 1, 2, 3))
            for owner, oz in here:
                if abs(oz) == 3:
                    pass_on(owner, oz, j, c, (0, 1))
        for j in (0, 1):
            pass_on(c, 0, j, c)
        stage(0, (3, -3))
        stage(0, (1, -1))
        stage(1, (3, -3))
        stage(1, (1, -1))
        stage(0, (2, -2, 4, -4))
        stage(0, (6, -6))
        stage(1, (2, -2, 4, -4))
        stage(1, (6, -6))
        leaves_complete(c, 0)

    def leaves_complete(c, j):
        for oz, dy in sorted(HELD, key=lambda h: abs(h[0]) + h[1]):
            if dy or oz not in INNER or carrier(c, oz) != c:
                arrived(oz, dy, j)

    on_cores(relay_blocks)
    for c in loads[2:]:
        c.wait()
    xs[...] = buf[:, 0].astype(F32).reshape(xs.shape).astype(BF16)

    half = xs.shape[0] // 2
    mine = pl.ds(pl.multiple_of(core * half, half), half)
    theirs = pl.ds(pl.multiple_of((1 - core) * half, half), half)
    last = (((1,), (1,)), ((), ()))

    def product(k, at):
        rows_of, weight = ((xs, wg), (xs, wu), (ys, wd))[k]
        return lax.dot_general(rows_of[at, :], weight[...], last, preferred_element_type=F32)

    chips = slabs.shape[1]
    share = half // chips
    def to_mate(k):
        far[k] = product(k, theirs)
        send(far.at[k], got.at[k], cs_sem.at[k], cr_sem.at[k], mate)

    on_cores(all_ready)
    to_mate(0)
    to_mate(1)
    own[0] = product(0, mine)
    for k in range(3):
        copy_to(far.at[k], got.at[k], cs_sem.at[k], cr_sem.at[k], mate).wait_recv()
        total = own[k] + got[k]
        own[k] = total
        slabs[k] = total.reshape(chips, share, -1).astype(BF16)
        for i, (a, b) in enumerate(others):
            chip = chip_at(a, b)
            send(slabs.at[k, chip], landed.at[i, k], ts_sem.at[i, k], tr_sem.at[i, k],
                 (s, chip * 2 + core))
        if k == 0:
            own[1] = product(1, mine)
        if k == 1:
            on_cores(lambda c: leaves_complete(c, 1))
            ys[...] = buf[:, 1].astype(F32).reshape(ys.shape).astype(BF16)
            to_mate(2)
            own[2] = product(2, mine)
    done()
    me = chip_at(0, 0)
    at = core * chips + me
    sums = []
    for k in range(3):
        total = own[k, pl.ds(pl.multiple_of(me * share, share), share), :]
        for i in reversed(range(len(others))):
            copy_to(slabs.at[k, 0], landed.at[i, k], ts_sem.at[i, k], tr_sem.at[i, k], mate).wait_recv()
            total = total + landed[i, k].astype(F32)
        sums.append(total)
        if k == 1:
            gate, up = sums
            sig = jax.nn.sigmoid(gate)
            act[at, 0] = (gate * sig * up).astype(BF16)
    grad = sums[2]
    act[at, 1] = (grad * gate * sig).astype(BF16)
    act[at, 2] = (grad * up * sig * (1.0 + gate * (1.0 - sig))).astype(BF16)

    def units_of(g, late):
        return act.at[g, 0] if late else act.at[g, pl.ds(1, 2)]

    def give_units(late):
        ref = units_of(at, late)
        for i, chip in enumerate(chips_at):
            send(ref, ref, as_sem.at[i, late], ar_sem.at[i, late], (s, chip * 2 + core))
        send(ref, ref, bs_sem.at[7, late], br_sem.at[7, late], mate)

    from_chips = [chip_at(-a, b) for a, b in others] + [me]

    def hand_over_units(late):
        for i in reversed(range(len(others))):
            ref = units_of(core * chips + from_chips[i], late)
            copy_to(ref, ref, as_sem.at[i, late], ar_sem.at[i, late], mate).wait_recv()
            send(ref, ref, bs_sem.at[i, late], br_sem.at[i, late], mate)

    def units_complete(late):
        for i, chip in reversed(list(enumerate(from_chips))):
            ref = units_of((1 - core) * chips + chip, late)
            copy_to(ref, ref, bs_sem.at[i, late], br_sem.at[i, late], mate).wait_recv()

    give_units(0)
    give_units(1)
    hand_over_units(0)
    units_complete(0)

    tokens, units = xs.shape[0], wg.shape[0]
    gate_unit = act[:, 2].reshape(tokens, units)
    up_unit = act[:, 1].reshape(tokens, units)
    term = jnp.dot(gate_unit, wg[...], preferred_element_type=F32)
    term = term + jnp.dot(up_unit, wu[...], preferred_element_type=F32)
    dxp[...] = term.reshape(dxp.shape)

    leaves[...] = term.reshape(dxp.shape).astype(BF16)
    first = (((0,), (0,)), ((), ()))
    def send_up(key, by):
        c, oz, dy, kind = key
        up, dz, _ = UP[key]
        target = (seq_at(-dz, dy), tp_of(carrier(c, up)))
        if key in INNER_KEYS:
            n = INNER_KEYS.index(key)
            issue(by, lambda: copy_to(zsend.at[n], zrecv.at[n], fzs_sem.at[n], fzr_sem.at[n], target))
        else:
            n = LEAF_KEYS.index(key)
            issue(by, lambda: copy_to(side(leaves.at[seq_at(-oz, dy)], oz), side(lrecv.at[n], oz),
                                      fys_sem.at[n], fyr_sem.at[n], target))

    def collected(c, oz):
        kind = "R" if carrier(c, oz) != c else "M"
        value = jnp.zeros((rows, depth), F32) if kind == "R" else dxp[seq_at(-oz)]
        edges = inward(c, oz)
        for dz, dy, to in sorted(edges, key=lambda e: abs(e[0])) if oz == 0 else edges[::-1]:
            key = (c, oz + dz, dy, to)
            if key in INNER_KEYS:
                n = INNER_KEYS.index(key)
                copy_to(zsend.at[n], zrecv.at[n], fzs_sem.at[n], fzr_sem.at[n], across).wait_recv()
                value = value + zrecv[n]
            else:
                n = LEAF_KEYS.index(key)
                ref = side(lrecv.at[n], key[1])
                copy_to(ref, ref, fys_sem.at[n], fyr_sem.at[n], across).wait_recv()
                nothing = jnp.zeros((rows, wide), F32)
                if key[1] == 8:
                    value = value + jnp.concatenate([lrecv[n, :, :wide].astype(F32), nothing], axis=1)
                elif key[1] == -8:
                    value = value + jnp.concatenate([nothing, lrecv[n, :, wide:].astype(F32)], axis=1)
                else:
                    value = value + lrecv[n].astype(F32)
        return value

    def forward(c, oz, by):
        key = (c, oz, 0, "R" if carrier(c, oz) != c else "M")
        zsend[INNER_KEYS.index(key)] = collected(c, oz)
        send_up(key, by)

    urgent = (8, 7, 5, 6, 4, 2, 3, 1, 0)

    def start_leaves(c):
        mine = [k for k in LEAF_KEYS if k[0] == c]
        for key in sorted(mine, key=lambda k: (urgent.index(abs(k[1])), -k[2])):
            send_up(key, c)

    def middle(c):
        for oz in (4, -4, 2, -2):
            forward(c, oz, c)

    def inner(c):
        for oz in (1, -1):
            forward(c, oz, c)

    def outer(c):
        for b in ((1, 0) if c else ()):
            for oz in (6, -6):
                forward(b, oz, c)

    def three(c):
        for b in ((1, 0) if c else ()):
            for oz in (3, -3):
                forward(b, oz, c)

    def finish(c):
        dx_ref[...] = collected(c, 0).astype(BF16)

    on_cores(start_leaves)
    on_cores(outer)
    on_cores(middle)
    on_cores(inner)
    hand_over_units(1)
    gg[...] = lax.dot_general(gate_unit, xs[...], first, preferred_element_type=F32)
    ug[...] = lax.dot_general(up_unit, xs[...], first, preferred_element_type=F32)
    units_complete(1)
    dg[...] = lax.dot_general(act[:, 0].reshape(tokens, units), ys[...], first,
                              preferred_element_type=F32)
    on_cores(three)
    done()
    on_cores(finish)


def write_out(dx, gg, ug, dg, dx_out, gg_out, ug_out, dg_out, staged, sem):
    copies = [pltpu.make_async_copy(a, b, sem.at[i])
              for i, (a, b) in enumerate(((gg, gg_out), (ug, ug_out), (dg, dg_out)))]
    for c in copies:
        c.start()
    staged[...] = dx[...].reshape(staged.shape)
    copies.append(pltpu.make_async_copy(staged, dx_out, sem.at[3]))
    copies[3].start()
    for c in copies:
        c.wait()


def solution(mesh):
    nz = mesh.shape["seq"] // 2
    nx = mesh.shape["tp"] // 4
    chips = mesh.shape["tp"] // 2

    def per_device(inputs, out_grad, gate_weight, up_weight, down_weight):
        groups, local, depth = inputs.shape
        rows = groups * local
        units = gate_weight.shape[1]
        tokens = rows * mesh.shape["seq"]
        half, share = tokens // 2, tokens // (2 * chips)
        whole = pl.BlockSpec(memory_space=pltpu.VMEM)
        hbm = pl.BlockSpec(memory_space=pltpu.HBM)
        dma = pltpu.SemaphoreType.DMA
        vmem = pltpu.VMEM
        out = pl.pallas_call(
            lambda *refs: kernel(nz, nx, *refs),
            out_shape=(
                vmem((rows, depth), BF16),
                vmem((units, depth), F32), vmem((units, depth), F32), vmem((units, depth), F32),
            ),
            in_specs=[hbm] * 5,
            out_specs=(whole,) * 4,
            scratch_shapes=[
                vmem((groups, local, depth), BF16), vmem((groups, local, depth), BF16),
                vmem((2 * nz, 2, rows, depth), BF16), vmem((4, 2, rows, depth), BF16),
                vmem((units, depth), BF16), vmem((units, depth), BF16), vmem((units, depth), BF16),
                vmem((tokens, depth), BF16), vmem((tokens, depth), BF16),
                vmem((3, half, units), F32), vmem((3, half, units), F32),
                vmem((3, half, units), F32),
                vmem((3, chips, share, units), BF16),
                vmem((chips - 1, 3, share, units), BF16),
                vmem((2 * chips, 3, share, units), BF16),
                vmem((2 * nz, rows, depth), F32),
                vmem((2 * nz, rows, depth), BF16), vmem((len(LEAF_KEYS), rows, depth), BF16),
                vmem((len(INNER_KEYS), rows, depth), F32), vmem((len(INNER_KEYS), rows, depth), F32),
                pltpu.SemaphoreType.REGULAR, dma((5,)),
                dma((len(EDGES), 2)), dma((len(HELD), 2)), dma((4, 2)),
                dma((3,)), dma((3,)),
                dma((7, 3)), dma((7, 3)), dma((7, 2)), dma((7, 2)), dma((8, 2)), dma((8, 2)),
                dma((len(LEAF_KEYS),)), dma((len(LEAF_KEYS),)),
                dma((len(INNER_KEYS),)), dma((len(INNER_KEYS),)),
            ],
            compiler_params=pltpu.CompilerParams(
                collective_id=0, has_side_effects=True, vmem_limit_bytes=48 * 2**20),
        )(*[pltpu.with_memory_space_constraint(a, pltpu.HBM) for a in (
            inputs, out_grad, gate_weight.T, up_weight.T, down_weight)])
        grad = jax.ShapeDtypeStruct((units, depth), F32)
        dx, gg, ug, dg = pl.pallas_call(
            write_out,
            out_shape=(jax.ShapeDtypeStruct((groups, local, depth), BF16), grad, grad, grad),
            in_specs=[whole] * 4,
            out_specs=(hbm,) * 4,
            scratch_shapes=[vmem((groups, local, depth), BF16), dma((4,))],
            compiler_params=pltpu.CompilerParams(vmem_limit_bytes=8 * 2**20),
        )(*out)
        return dx, gg.T, ug.T, dg

    return jax.shard_map(
        per_device, mesh=mesh,
        in_specs=(P(None, "seq", "tp"), P(None, "seq", "tp"), P("tp", "seq"), P("tp", "seq"),
                  P("seq", "tp")),
        out_specs=(P(None, "seq", "tp"), P("tp", "seq"), P("tp", "seq"), P("seq", "tp")),
        check_vma=False)
```
